256 devices in a mesh: seq: 32 (over x, z), vocab: 8 (over y, core).
Axes of the slice: x: 4, y: 4, z: 8, core: 2. Of those that a mesh axis runs over, the one named last changes fastest.
Arguments:
- hidden: bfloat16 [32768, 3584], P('seq', 'vocab'), may hold values from -6 to 6
- norm_gain: float32 [3584], replicated, may hold values from 0.25 to 1.75
- head_weight: bfloat16 [3584, 8000], P(None, 'vocab'), may hold values from -0.3125 to 0.3125
- teacher_ids: int32 [32768, 128], P('seq'), may hold values from 0 to 7999
- teacher_probs: float32 [32768, 128], P('seq'), may hold values from 0.0001 to 0.015
- doc_ids: int32 [32768], P('seq'), may hold values from -1 to 127, as said below
- plan: int32 [256, 2], P('seq'), may hold values from -1 to 31, as said below
Outputs:
- doc_loss: float32 [128], replicated
- row_lse: float32 [16384], P('seq')
The draws below stay inside these ranges and needn't reach their ends.
Inputs may be any that keep to these rules, and one draw needn't show every extreme that they name: `plan`: row b of a seq index's 8 rows describes its home block b: a destination seq index and an owned slot 0 to 3 there, or -1 and -1 for a block without tokens. Live blocks of a seq index come first. Every owned slot of every seq index receives exactly one block, no seq index sends more than 1 block to one destination, and some seq index sends exactly 1 to some destination. `doc_ids`: -1 exactly on the rows of blocks without tokens. Over the live rows, taken seq index by seq index and in order, document numbers never fall; a document may be empty.
All inputs are finite; a program needn't handle non-finite values.
Results may differ from the reference program's by a relative error of at most 0.00035.
Values may be sent and summed in bfloat16 or wider, within the bound.
No kernel may reach another device: no remote copies, remote signals or barrier semaphores. Data moves between devices by JAX's collectives and lax.ppermute only.
A program may use at most 64 MiB of HBM per device.

```python
import math
import jax
import jax.numpy as jnp
import numpy as np
from jax import lax

D = 3584
TOPK = 128
BLOCK = 128
WORK = 4
BLK_DEV = 8
TOKENS = 32768
VOCAB = 8000
DOCS = 128
N_SEQ = 32


def plan_parts(key):
    base = jax.random.fold_in(key, 7001)
    pair_key, order_key, dest_key, slot_key, cut_key = jax.random.split(base, 5)
    halves = N_SEQ // 2
    first = jax.random.randint(pair_key, (halves,), 0, BLK_DEV + 1)
    first = first.at[0].set(BLK_DEV)
    paired = jnp.stack([first, BLK_DEV - first], axis=1).reshape(-1)
    shuffle = jax.random.permutation(order_key, N_SEQ)
    active = paired[shuffle]
    offsets = jnp.cumsum(active) - active
    slots = jnp.arange(BLK_DEV, dtype=jnp.int32)
    alive = slots[None, :] < active[:, None]
    order = offsets[:, None] + slots[None, :]
    dest_perm = jax.random.permutation(dest_key, N_SEQ).astype(jnp.int32)
    target = dest_perm[order % N_SEQ]
    scores = jax.random.randint(slot_key, (N_SEQ, WORK), 0, 1 << 20) * WORK + jnp.arange(WORK, dtype=jnp.int32)[None, :]
    slot_perm = jnp.argsort(scores, axis=1).astype(jnp.int32)
    rank = jnp.clip(order // N_SEQ, 0, WORK - 1)
    owner_slot = slot_perm[target, rank]
    plan = jnp.stack([jnp.where(alive, target, -1), jnp.where(alive, owner_slot, -1)], axis=-1)
    plan = plan.reshape(N_SEQ * BLK_DEV, 2).astype(jnp.int32)
    live_rows = WORK * N_SEQ * BLOCK
    cuts = jnp.sort(jax.random.randint(cut_key, (DOCS - 1,), 1, live_rows))
    position = order[:, :, None] * BLOCK + jnp.arange(BLOCK, dtype=jnp.int32)[None, None, :]
    labels = jnp.searchsorted(cuts, position.reshape(-1), side='right').astype(jnp.int32)
    row_alive = jnp.repeat(alive.reshape(-1), BLOCK)
    documents = jnp.where(row_alive, labels, -1).astype(jnp.int32)
    return (plan, documents)


def draw_plan(key, part):
    return plan_parts(key)[0]


def draw_doc_ids(key, part):
    return plan_parts(key)[1]


def with_ends(result, own_key, least, top_value):
    index_at = [jax.random.randint(jax.random.fold_in(own_key, axis), (), 0, length) for axis, length in enumerate(result.shape)]
    main_axis = result.shape.index(max(result.shape))
    neighbour = index_at[:main_axis] + [(index_at[main_axis] + 1) % result.shape[main_axis]] + index_at[main_axis + 1:]
    return result.at[tuple(index_at)].set(least).at[tuple(neighbour)].set(top_value)


def block_scale(stream_key, extent, shards, smallest, top_value):
    loudness = 1.0
    for dim, blocks in shards:
        heights = jax.random.uniform(jax.random.fold_in(jax.random.fold_in(stream_key, 6), dim), (blocks,), jnp.float32, smallest / len(shards), top_value / len(shards))
        loudness = loudness * jnp.repeat(jnp.exp(heights), extent[dim] // blocks).reshape((-1,) + (1,) * (len(extent) - 1 - dim))
    return loudness


def cumulative_ranks(amount, skew):
    portions = [(1 << 20) // math.isqrt(grade ** skew) + 1 for grade in range(1, amount + 1)]
    deviation = 1 + sum(portions) // (1 << 30)
    return np.cumsum(np.array([max(1, weight // deviation) for weight in portions]))


def skewed_ids(stream_key, shape, amount, lean):
    table = cumulative_ranks(amount, lean)
    pick = jax.random.randint(jax.random.fold_in(stream_key, 1), shape, 0, int(table[amount - 1]))
    rank = jnp.searchsorted(jnp.asarray(table, jnp.int32), pick, side="right")
    return jax.random.permutation(jax.random.fold_in(stream_key, 2), amount)[rank].astype(jnp.int32)


def centred(rng, extent, deviation, reach, cuts=(), kind=jnp.bfloat16):
    result = deviation * jax.random.normal(rng, extent, jnp.float32)
    if cuts:
        result = result * block_scale(rng, extent, cuts, -0.22, 0.18)
    return jnp.clip(result, -reach, reach).astype(kind)


def setup_inputs(seed: int = 0) -> dict:
    keys = jax.random.split(jax.random.key(seed), 8)
    hidden = centred(keys[0], (TOKENS, D), 1.0, 6.0, ((0, 32), (1, 8)))
    norm_gain = jnp.clip(1.0 + 0.15 * jax.random.normal(keys[1], (D,), jnp.float32), 0.25, 1.75)
    head_weight = centred(keys[2], (D, VOCAB), (D // 9) ** -0.5, 0.3125, ((1, 8),))
    teacher_ids = with_ends(skewed_ids(keys[3], (TOKENS, TOPK), VOCAB, 1), jax.random.fold_in(keys[3], 3), 0, VOCAB - 1).astype(jnp.int32)
    teacher_probs = jnp.clip(jnp.exp(math.log(0.015) - 5.0106353 * jax.random.uniform(keys[4], (TOKENS, TOPK), jnp.float32) ** block_scale(keys[4], (TOKENS, TOPK), ((0, 32),), -0.2, 0.2)), 0.0001, 0.015)
    doc_ids = draw_doc_ids(jax.random.fold_in(keys[7], 71), 0)
    plan = draw_plan(jax.random.fold_in(keys[7], 71), 0)
    return {"hidden": hidden, "norm_gain": norm_gain, "head_weight": head_weight, "teacher_ids": teacher_ids, "teacher_probs": teacher_probs, "doc_ids": doc_ids, "plan": plan}


SOFTCAP = 30.0
EPS = 1e-06

def block_losses(pieces, norm_gain, head_weight):
    rows_in, ids_in, probs_in = pieces
    values = rows_in.astype(jnp.float32)
    inverse = lax.rsqrt(lax.optimization_barrier(jnp.mean(values * values, axis=-1, keepdims=True)) + EPS)
    normed = (values * inverse * norm_gain).astype(jnp.bfloat16)
    logits = jnp.dot(normed, head_weight, preferred_element_type=jnp.float32)
    capped = SOFTCAP * jnp.tanh(logits / SOFTCAP)
    log_total = jnp.log(lax.optimization_barrier(jnp.sum(jnp.exp(capped), axis=-1)))
    chosen = jnp.take_along_axis(capped, ids_in, axis=1)
    picked = lax.optimization_barrier(jnp.sum(probs_in * chosen, axis=-1))
    return (log_total, log_total * lax.optimization_barrier(jnp.sum(probs_in, axis=-1)) - picked)

def reference(hidden, norm_gain, head_weight, teacher_ids, teacher_probs, doc_ids, plan):
    owned_blocks = N_SEQ * WORK
    target = plan[:, 0]
    place = jnp.where(target >= 0, target * WORK + plan[:, 1], owned_blocks).astype(jnp.int32)
    home_index = jnp.arange(plan.shape[0], dtype=jnp.int32)
    source = jnp.zeros((owned_blocks,), jnp.int32).at[place].set(home_index, mode='drop')
    features = hidden.shape[1]
    row_total = owned_blocks * BLOCK
    block_rows = math.gcd(row_total, 512)
    owned_rows = hidden.reshape(-1, BLOCK, features)[source].reshape(-1, block_rows, features)
    owned_ids = teacher_ids.reshape(-1, BLOCK, TOPK)[source].reshape(-1, block_rows, TOPK)
    owned_probs = teacher_probs.reshape(-1, BLOCK, TOPK)[source].reshape(-1, block_rows, TOPK)
    log_total, row_loss = lax.map(lambda pieces: block_losses(pieces, norm_gain, head_weight), (owned_rows, owned_ids, owned_probs))
    row_lse = log_total.reshape(-1)
    flat_loss = row_loss.reshape(-1)
    owned_docs = doc_ids.reshape(-1, BLOCK)[source].reshape(-1)
    totals = jax.ops.segment_sum(flat_loss, owned_docs, num_segments=DOCS)
    counts = jax.ops.segment_sum(jnp.ones_like(flat_loss), owned_docs, num_segments=DOCS)
    doc_loss = totals / jnp.maximum(counts, 1.0)
    return (doc_loss, row_lse)
```

```python
import functools

import jax
import jax.numpy as jnp
from jax import lax
from jax.experimental import pallas as pl
from jax.experimental.pallas import tpu as pltpu
from jax.sharding import PartitionSpec as P

BLOCK = 128
WORK = 4
DOCS = 128
CHIPS = 4
CORES = 2
CHUNKS = 2
SOFTCAP = 30.0
EPS = 1e-06
LANES = 128
MIB = 1 << 20


def on_diagonal():
    lane = lax.broadcasted_iota(jnp.int32, (BLOCK, LANES), 1)
    return lane == lax.broadcasted_iota(jnp.int32, (BLOCK, LANES), 0)


def as_row(column):
    return jnp.sum(jnp.where(on_diagonal(), column, 0.0), axis=0, keepdims=True)


def head_kernel(chunk, where_ref, weight_ref, ids_ref, probs_ref, *refs):
    count = 2 * (CHIPS + 1)
    pieces, refs = refs[:count], refs[count:]
    earlier = refs[0] if chunk else None
    outs, (rows_ref, logits_ref, scale_ref) = refs[bool(chunk) : -3], refs[-3:]
    chip, core, offset = where_ref[0], where_ref[1], where_ref[2]
    vocab, features = weight_ref.shape
    shard, width = pieces[0].shape
    half = width // 2

    squares = [jnp.zeros((16, half), jnp.float32) for _ in range(2)]
    for side in range(2):
        base = side * (CHIPS + 1)
        for hop, parts in ((0, (0,)), (3, (1,)), (1, (2,)), (2, (3, 4))):
            owner = lax.rem(chip + hop, CHIPS) * CORES + (core if side == 0 else 1 - core)
            start = pl.multiple_of(owner * shard, 64)

            def move(i, carry):
                low, high = carry
                at = pl.multiple_of(i * 16, 16)
                if len(parts) == 1:
                    both = pieces[base + parts[0]][pl.ds(at, 16), :]
                    left, right = both[:, :half], both[:, half:]
                else:
                    left = pieces[base + parts[0]][pl.ds(at, 16), :]
                    right = pieces[base + parts[1]][pl.ds(at, 16), :]
                to = pl.ds(pl.multiple_of(start + at, 16), 16)
                rows_ref[to, :half] = left
                rows_ref[to, half:] = right
                left, right = left.astype(jnp.float32), right.astype(jnp.float32)
                return low + left * left, high + right * right

            squares = lax.fori_loop(0, shard // 16, move, tuple(squares), unroll=4)
    for side in range(2):
        mean = jnp.sum(squares[side], axis=0, keepdims=True) * (1.0 / features)
        scale = lax.rsqrt(mean + EPS) * (1.0 / SOFTCAP)
        scale_ref[:, side * half : (side + 1) * half] = jnp.broadcast_to(scale, (8, half))

    logits_ref[...] = jnp.dot(
        weight_ref[...], rows_ref[...], preferred_element_type=jnp.float32
    )

    blocks = width // BLOCK
    expsums, picks = [], []
    for q in range(blocks):
        lanes = slice(q * BLOCK, (q + 1) * BLOCK)
        scale = scale_ref[0:1, lanes]
        rows = slice((chunk * blocks + q) * BLOCK, (chunk * blocks + q + 1) * BLOCK)
        within = ids_ref[rows, :] - offset
        tile, spot = within >> 7, within & (LANES - 1)
        sums = jnp.zeros((8, BLOCK), jnp.float32)
        chosen = jnp.zeros((BLOCK, LANES), jnp.float32)
        for t in range(-(-vocab // LANES)):
            size = min(LANES, vocab - t * LANES)
            soft = jnp.tanh(logits_ref[t * LANES : t * LANES + size, lanes] * scale)
            power = jnp.exp(SOFTCAP * soft)
            sums = sums + jnp.sum(power.reshape(size // 8, 8, BLOCK), axis=0)
            if size < LANES:
                soft = jnp.concatenate([soft, jnp.zeros((LANES - size, BLOCK), jnp.float32)], axis=0)
            found = jnp.take_along_axis(soft.T, spot, axis=1)
            chosen = jnp.where(tile == t, found, chosen)
        picked = SOFTCAP * jnp.sum(probs_ref[rows, :] * chosen, axis=1, keepdims=True)
        expsums.append(jnp.sum(sums, axis=0, keepdims=True))
        picks.append(as_row(picked))
    here = jnp.concatenate(expsums + picks, axis=0)
    if chunk == 0:
        stats_ref, mass_ref = outs
        stats_ref[...] = here
        for b in range(mass_ref.shape[0]):
            mass = jnp.sum(probs_ref[b * BLOCK : (b + 1) * BLOCK, :], axis=1, keepdims=True)
            mass_ref[b : b + 1, :] = as_row(mass)
    else:
        (copies_ref,) = outs
        before = earlier[...]
        for k in range(copies_ref.shape[0]):
            copies_ref[k, 0:blocks] = before[:blocks]
            copies_ref[k, blocks : 2 * blocks] = here[:blocks]
            copies_ref[k, 2 * blocks : 3 * blocks] = before[blocks:]
            copies_ref[k, 3 * blocks :] = here[blocks:]


def head(chunk, where, weight, ids, probs, pieces, earlier, peers):
    vocab, features = weight.shape
    width = pieces[0].shape[1]
    blocks = ids.shape[0] // BLOCK
    stat = lambda *shape: jax.ShapeDtypeStruct(shape, jnp.float32)
    if chunk == 0:
        out_shape = (stat(blocks, BLOCK), stat(blocks, BLOCK))
    else:
        out_shape = (stat(peers, 2 * blocks, BLOCK),)
    vmem = pl.BlockSpec(memory_space=pltpu.VMEM)
    operands = [weight, ids, probs, *pieces] + ([earlier] if chunk else [])
    return pl.pallas_call(
        functools.partial(head_kernel, chunk),
        out_shape=out_shape,
        in_specs=[pl.BlockSpec(memory_space=pltpu.SMEM)] + [vmem] * len(operands),
        out_specs=(vmem,) * len(out_shape),
        scratch_shapes=[
            pltpu.VMEM((features, width), jnp.bfloat16),
            pltpu.VMEM((vocab, width), jnp.float32),
            pltpu.VMEM((8, width), jnp.float32),
        ],
        compiler_params=pltpu.CompilerParams(vmem_limit_bytes=28 * MIB),
        cost_estimate=pl.CostEstimate(
            flops=2 * vocab * features * width,
            bytes_accessed=2 * (weight.size + features * width),
            transcendentals=2 * vocab * width,
        ),
        name="head",
    )(where, *operands)


def losses_kernel(plan_ref, came_ref, mass_ref, docs_ref, message_ref):
    blocks = mass_ref.shape[0]
    sums = jnp.sum(came_ref[...], axis=0)
    expsum, picked = sums[:blocks], sums[blocks:]
    alive = docs_ref[...] >= 0
    lse = jnp.log(jnp.where(alive, expsum, 1.0))
    row_loss = jnp.where(alive, lse * mass_ref[...] - picked, 0.0)
    label = lax.broadcasted_iota(jnp.int32, (DOCS, LANES), 0)
    totals = jnp.zeros((DOCS, LANES), jnp.float32)
    counts = jnp.zeros((DOCS, LANES), jnp.float32)
    for b in range(blocks):
        member = label == docs_ref[b : b + 1, :]
        totals = totals + jnp.where(member, row_loss[b : b + 1, :], 0.0)
        counts = counts + jnp.where(member, 1.0, 0.0)
    totals = as_row(jnp.sum(totals, axis=1, keepdims=True))
    counts = as_row(jnp.sum(counts, axis=1, keepdims=True))
    peers = message_ref.shape[0]
    peer = lax.broadcasted_iota(jnp.int32, (peers, LANES), 0)
    routed = jnp.zeros((peers, LANES), jnp.float32)
    mark = jnp.zeros((peers, LANES), jnp.int32)
    for b in range(blocks):
        chosen = peer == plan_ref[0, b]
        routed = jnp.where(chosen, lse[b : b + 1, :], routed)
        mark = jnp.where(chosen, plan_ref[1, b] + 1, mark)
    message_ref[:, 0 * LANES : 1 * LANES] = routed
    message_ref[:, 1 * LANES : 2 * LANES] = jnp.broadcast_to(totals, (peers, LANES))
    message_ref[:, 2 * LANES : 3 * LANES] = jnp.broadcast_to(counts, (peers, LANES))
    message_ref[:, 3 * LANES : 4 * LANES] = mark.astype(jnp.float32)


def losses(plan, came, mass, docs, peers):
    vmem = pl.BlockSpec(memory_space=pltpu.VMEM)
    return pl.pallas_call(
        losses_kernel,
        out_shape=jax.ShapeDtypeStruct((peers, 4 * LANES), jnp.float32),
        in_specs=[pl.BlockSpec(memory_space=pltpu.SMEM), vmem, vmem, vmem],
        out_specs=vmem,
        compiler_params=pltpu.CompilerParams(vmem_limit_bytes=8 * MIB),
        name="losses",
    )(plan, came, mass, docs)


def finish_kernel(came_ref, doc_ref, lse_ref):
    mark = came_ref[:, 3 * LANES : 4 * LANES]
    came = came_ref[:, 0:LANES]
    for s in range(WORK):
        lse_ref[s : s + 1, :] = jnp.sum(
            jnp.where(mark == float(s + 1), came, 0.0), axis=0, keepdims=True
        )
    totals = jnp.sum(came_ref[:, LANES : 2 * LANES], axis=0, keepdims=True)
    counts = jnp.sum(came_ref[:, 2 * LANES : 3 * LANES], axis=0, keepdims=True)
    doc_ref[...] = totals / jnp.maximum(counts, 1.0)


def finish(came):
    vmem = pl.BlockSpec(memory_space=pltpu.VMEM)
    stat = lambda rows: jax.ShapeDtypeStruct((rows, LANES), jnp.float32)
    return pl.pallas_call(
        finish_kernel,
        out_shape=(stat(1), stat(WORK)),
        in_specs=[vmem],
        out_specs=(vmem, vmem),
        compiler_params=pltpu.CompilerParams(vmem_limit_bytes=8 * MIB),
        name="finish",
    )(came)


def turn(step):
    count = CORES * CHIPS
    return [(i, (i + CORES * step) % count) for i in range(count)]


SWAP = [(i, i ^ 1) for i in range(CORES * CHIPS)]


def move(x, pairs):
    return lax.ppermute(x, "vocab", pairs)


def per_device(hidden, norm_gain, head_weight, teacher_ids, teacher_probs, doc_ids, plan):
    seq_count, peers = lax.axis_size("seq"), lax.axis_size("vocab")
    vocab_local = head_weight.shape[1]
    shard = lax.axis_index("vocab")
    where = jnp.stack([shard // CORES, shard % CORES, shard * vocab_local]).astype(jnp.int32)
    weight = (head_weight.T.astype(jnp.float32) * norm_gain[None, :]).astype(jnp.bfloat16)

    turned = hidden.T
    width = turned.shape[1] // CHUNKS
    half = width // 2
    here = [turned[:, k * width : (k + 1) * width] for k in range(CHUNKS)]
    near = [(move(x, turn(1)), move(x, turn(-1))) for x in here]
    far = [(move(up[:, :half], turn(1)), move(down[:, half:], turn(-1))) for up, down in near]
    earlier = mass = None
    for k in range(CHUNKS):
        own = (here[k], *near[k], *far[k])
        pieces = own + tuple(move(x, SWAP) for x in own)
        outs = head(k, where, weight, teacher_ids, teacher_probs, pieces, earlier, peers)
        if k == 0:
            earlier, mass = outs
    (copies,) = outs

    came = lax.all_to_all(copies, "vocab", split_axis=0, concat_axis=0, tiled=True)
    message = losses(plan.T, came, mass, doc_ids.reshape(-1, BLOCK), seq_count)
    came = lax.all_to_all(message, "seq", split_axis=0, concat_axis=0, tiled=True)
    doc_loss, row_lse = finish(came)
    return (doc_loss.reshape(-1), row_lse.reshape(-1))


def solution(mesh):
    return jax.shard_map(
        per_device,
        mesh=mesh,
        in_specs=(
            P("seq", "vocab"),
            P(),
            P(None, "vocab"),
            P("seq", None),
            P("seq", None),
            P("seq"),
            P("seq", None),
        ),
        out_specs=(P(), P("seq")),
        check_vma=False,
    )
```

```python
import functools

import jax
import jax.numpy as jnp
from jax import lax
from jax.experimental import pallas as pl
from jax.experimental.pallas import tpu as pltpu
from jax.sharding import PartitionSpec as P


BLOCK = 128
WORK = 4
DOCS = 128
CHIPS = 4
CORES = 2
CHUNKS = 2
HOPS = (0, 1, 3, 2)
SOFTCAP = 30.0
EPS = 1e-06
LANES = 128
MIB = 1 << 20


def on_diagonal():
    lane = lax.broadcasted_iota(jnp.int32, (BLOCK, LANES), 1)
    return lane == lax.broadcasted_iota(jnp.int32, (BLOCK, LANES), 0)


def as_row(column):
    return jnp.sum(jnp.where(on_diagonal(), column, 0.0), axis=0, keepdims=True)


def prepare_kernel(where_ref, weight_ref, gain_ref, out_ref, *scratch):
    parts, sems = scratch[:-1], scratch[-1]
    width = parts[0].shape[1]
    tiles = width // LANES
    chips = [lax.rem(where_ref[0] + hop, CHIPS) for hop in HOPS]
    copies = []
    for k, chip in enumerate(chips):
        start = pl.multiple_of(chip * width, LANES)
        copies.append(
            pltpu.make_async_copy(weight_ref.at[:, pl.ds(start, width)], parts[k], sems.at[k])
        )
        copies[k].start()
    for k, chip in enumerate(chips):
        copies[k].wait()
        for t in range(tiles):
            gain = gain_ref[pl.ds(chip * tiles + t, 1), :]
            part = parts[k][:, t * LANES : (t + 1) * LANES].astype(jnp.float32) * gain
            to = k * width + t * LANES
            out_ref[:, to : to + LANES] = part.astype(jnp.bfloat16)


def prepare(where, weight, gain):
    vmem = pl.BlockSpec(memory_space=pltpu.VMEM)
    vocab, features = weight.shape
    return pl.pallas_call(
        prepare_kernel,
        out_shape=jax.ShapeDtypeStruct(weight.shape, jnp.bfloat16),
        in_specs=[
            pl.BlockSpec(memory_space=pltpu.SMEM),
            pl.BlockSpec(memory_space=pltpu.HBM),
            vmem,
        ],
        out_specs=vmem,
        scratch_shapes=[pltpu.VMEM((vocab, features // CHIPS), jnp.bfloat16)] * CHIPS
        + [pltpu.SemaphoreType.DMA((CHIPS,))],
        compiler_params=pltpu.CompilerParams(vmem_limit_bytes=24 * MIB),
        cost_estimate=pl.CostEstimate(
            flops=500 * weight.size, bytes_accessed=4 * weight.size, transcendentals=0
        ),
        name="prepare",
    )(where, weight, gain)


def stack(core, pieces, rows_ref):
    shard, width = pieces[0].shape
    squares = jnp.zeros((16, width), jnp.float32)
    for k, piece in enumerate(pieces):
        pair, side = k // CORES, k % CORES
        start = pair * CORES * shard + (core if side == 0 else 1 - core) * shard

        def step(i, carry):
            at = pl.multiple_of(i * 16, 16)
            part = piece[pl.ds(at, 16), :]
            rows_ref[pl.ds(pl.multiple_of(start + at, 16), 16), :] = part
            wide = part.astype(jnp.float32)
            return carry + wide * wide

        squares = lax.fori_loop(0, shard // 16, step, squares, unroll=4)
    return squares


def near_kernel(where_ref, weight_ref, *refs):
    pieces, (logits_ref, squares_ref, rows_ref) = refs[:-3], refs[-3:]
    squares_ref[...] = stack(where_ref[1], pieces, rows_ref)
    logits_ref[...] = jnp.dot(
        weight_ref[:, : rows_ref.shape[0]], rows_ref[...], preferred_element_type=jnp.float32
    )


def near_head(where, weight, pieces):
    vocab, _ = weight.shape
    shard, width = pieces[0].shape
    depth = shard * len(pieces)
    vmem = pl.BlockSpec(memory_space=pltpu.VMEM)
    return pl.pallas_call(
        near_kernel,
        out_shape=(
            jax.ShapeDtypeStruct((vocab, width), jnp.float32),
            jax.ShapeDtypeStruct((16, width), jnp.float32),
        ),
        in_specs=[pl.BlockSpec(memory_space=pltpu.SMEM)] + [vmem] * (1 + len(pieces)),
        out_specs=(vmem, vmem),
        scratch_shapes=[pltpu.VMEM((depth, width), jnp.bfloat16)],
        compiler_params=pltpu.CompilerParams(vmem_limit_bytes=24 * MIB),
        cost_estimate=pl.CostEstimate(
            flops=2 * vocab * depth * width,
            bytes_accessed=2 * (vocab + width) * depth,
            transcendentals=0,
        ),
        name="near",
    )(where, weight, *pieces)


def far_kernel(chunk, features, count, where_ref, weight_ref, near_ref, squares_ref, ids_ref, probs_ref, *refs):
    pieces, refs = refs[:count], refs[count:]
    earlier = refs[0] if chunk else None
    outs, (rows_ref, logits_ref, scale_ref) = refs[bool(chunk) : -3], refs[-3:]
    vocab, depth = weight_ref.shape[0], rows_ref.shape[0]
    width = rows_ref.shape[1]
    squares = squares_ref[...] + stack(where_ref[1], pieces, rows_ref)
    mean = jnp.sum(squares, axis=0, keepdims=True) * (1.0 / features)
    scale = lax.rsqrt(mean + EPS) * (1.0 / SOFTCAP)
    scale_ref[...] = jnp.broadcast_to(scale, scale_ref.shape)
    logits_ref[...] = near_ref[...] + jnp.dot(
        weight_ref[:, features - depth :], rows_ref[...], preferred_element_type=jnp.float32
    )

    blocks = width // BLOCK
    expsums, picks = [], []
    for q in range(blocks):
        lanes = slice(q * BLOCK, (q + 1) * BLOCK)
        scale = scale_ref[0:1, lanes]
        rows = slice((chunk * blocks + q) * BLOCK, (chunk * blocks + q + 1) * BLOCK)
        within = ids_ref[rows, :] - where_ref[2]
        tile, spot = within >> 7, within & (LANES - 1)
        sums = jnp.zeros((8, BLOCK), jnp.float32)
        turned = []
        for t in range(-(-vocab // LANES)):
            size = min(LANES, vocab - t * LANES)
            soft = jnp.tanh(logits_ref[t * LANES : t * LANES + size, lanes] * scale)
            power = jnp.exp(SOFTCAP * soft)
            sums = sums + jnp.sum(power.reshape(size // 8, 8, BLOCK), axis=0)
            if size < LANES:
                soft = jnp.concatenate([soft, jnp.zeros((LANES - size, BLOCK), jnp.float32)], axis=0)
            turned.append(soft.T)
        chosen = []
        for g in range(0, BLOCK, 8):
            found = jnp.zeros((8, LANES), jnp.float32)
            for t, soft in enumerate(turned):
                part = jnp.take_along_axis(
                    soft[g : g + 8], spot[g : g + 8], axis=1, mode="promise_in_bounds"
                )
                found = jnp.where(tile[g : g + 8] == t, part, found)
            chosen.append(found)
        chosen = jnp.concatenate(chosen, axis=0)
        picked = SOFTCAP * jnp.sum(probs_ref[rows, :] * chosen, axis=1, keepdims=True)
        expsums.append(jnp.sum(sums, axis=0, keepdims=True))
        picks.append(as_row(picked))
    here = jnp.concatenate(expsums + picks, axis=0)
    if chunk == 0:
        stats_ref, mass_ref = outs
        stats_ref[...] = here
        for b in range(mass_ref.shape[0]):
            mass = jnp.sum(probs_ref[b * BLOCK : (b + 1) * BLOCK, :], axis=1, keepdims=True)
            mass_ref[b : b + 1, :] = as_row(mass)
    else:
        (copies_ref,) = outs
        before = earlier[...]
        for k in range(copies_ref.shape[0]):
            copies_ref[k, 0:blocks] = before[:blocks]
            copies_ref[k, blocks : 2 * blocks] = here[:blocks]
            copies_ref[k, 2 * blocks : 3 * blocks] = before[blocks:]
            copies_ref[k, 3 * blocks :] = here[blocks:]


def far_head(chunk, where, weight, near, squares, ids, probs, pieces, earlier, peers):
    vocab, features = weight.shape
    shard, width = pieces[0].shape[0], near.shape[1]
    blocks = ids.shape[0] // BLOCK
    stat = lambda *shape: jax.ShapeDtypeStruct(shape, jnp.float32)
    if chunk == 0:
        out_shape = (stat(blocks, BLOCK), stat(blocks, BLOCK))
    else:
        out_shape = (stat(peers, 2 * blocks, BLOCK),)
    vmem = pl.BlockSpec(memory_space=pltpu.VMEM)
    operands = [weight, near, squares, ids, probs, *pieces] + ([earlier] if chunk else [])
    depth = len(pieces) * shard
    return pl.pallas_call(
        functools.partial(far_kernel, chunk, features, len(pieces)),
        out_shape=out_shape,
        in_specs=[pl.BlockSpec(memory_space=pltpu.SMEM)] + [vmem] * len(operands),
        out_specs=(vmem,) * len(out_shape),
        scratch_shapes=[
            pltpu.VMEM((depth, width), jnp.bfloat16),
            pltpu.VMEM((vocab, width), jnp.float32),
            pltpu.VMEM((8, width), jnp.float32),
        ],
        compiler_params=pltpu.CompilerParams(vmem_limit_bytes=24 * MIB),
        cost_estimate=pl.CostEstimate(
            flops=2 * 2 * vocab * depth * width,
            bytes_accessed=2 * (vocab + width) * depth + 8 * vocab * width,
            transcendentals=2 * vocab * width,
        ),
        name="far",
    )(where, *operands)


def losses_kernel(plan_ref, came_ref, mass_ref, docs_ref, message_ref):
    blocks = mass_ref.shape[0]
    sums = jnp.sum(came_ref[...], axis=0)
    expsum, picked = sums[:blocks], sums[blocks:]
    alive = docs_ref[...] >= 0
    lse = jnp.log(jnp.where(alive, expsum, 1.0))
    row_loss = jnp.where(alive, lse * mass_ref[...] - picked, 0.0)
    label = lax.broadcasted_iota(jnp.int32, (DOCS, LANES), 0)
    totals = jnp.zeros((DOCS, LANES), jnp.float32)
    counts = jnp.zeros((DOCS, LANES), jnp.float32)
    for b in range(blocks):
        member = label == docs_ref[b : b + 1, :]
        totals = totals + jnp.where(member, row_loss[b : b + 1, :], 0.0)
        counts = counts + jnp.where(member, 1.0, 0.0)
    totals = as_row(jnp.sum(totals, axis=1, keepdims=True))
    counts = as_row(jnp.sum(counts, axis=1, keepdims=True))
    peers = message_ref.shape[0]
    peer = lax.broadcasted_iota(jnp.int32, (peers, LANES), 0)
    routed = jnp.zeros((peers, LANES), jnp.float32)
    mark = jnp.zeros((peers, LANES), jnp.int32)
    for b in range(blocks):
        chosen = peer == plan_ref[0, b]
        routed = jnp.where(chosen, lse[b : b + 1, :], routed)
        mark = jnp.where(chosen, plan_ref[1, b] + 1, mark)
    message_ref[:, 0 * LANES : 1 * LANES] = routed
    message_ref[:, 1 * LANES : 2 * LANES] = jnp.broadcast_to(totals, (peers, LANES))
    message_ref[:, 2 * LANES : 3 * LANES] = jnp.broadcast_to(counts, (peers, LANES))
    message_ref[:, 3 * LANES : 4 * LANES] = mark.astype(jnp.float32)


def losses(plan, came, mass, docs, peers):
    vmem = pl.BlockSpec(memory_space=pltpu.VMEM)
    return pl.pallas_call(
        losses_kernel,
        out_shape=jax.ShapeDtypeStruct((peers, 4 * LANES), jnp.float32),
        in_specs=[pl.BlockSpec(memory_space=pltpu.SMEM), vmem, vmem, vmem],
        out_specs=vmem,
        compiler_params=pltpu.CompilerParams(vmem_limit_bytes=8 * MIB),
        name="losses",
    )(plan, came, mass, docs)


def finish_kernel(came_ref, doc_ref, lse_ref):
    mark = came_ref[:, 3 * LANES : 4 * LANES]
    came = came_ref[:, 0:LANES]
    for s in range(WORK):
        lse_ref[s : s + 1, :] = jnp.sum(
            jnp.where(mark == float(s + 1), came, 0.0), axis=0, keepdims=True
        )
    totals = jnp.sum(came_ref[:, LANES : 2 * LANES], axis=0, keepdims=True)
    counts = jnp.sum(came_ref[:, 2 * LANES : 3 * LANES], axis=0, keepdims=True)
    doc_ref[...] = totals / jnp.maximum(counts, 1.0)


def finish(came):
    vmem = pl.BlockSpec(memory_space=pltpu.VMEM)
    stat = lambda rows: jax.ShapeDtypeStruct((rows, LANES), jnp.float32)
    return pl.pallas_call(
        finish_kernel,
        out_shape=(stat(1), stat(WORK)),
        in_specs=[vmem],
        out_specs=(vmem, vmem),
        compiler_params=pltpu.CompilerParams(vmem_limit_bytes=8 * MIB),
        name="finish",
    )(came)


def turn(step):
    count = CORES * CHIPS
    return [(i, (i + CORES * step) % count) for i in range(count)]


SWAP = [(i, i ^ 1) for i in range(CORES * CHIPS)]


def move(x, pairs):
    return lax.ppermute(x, "vocab", pairs)


def per_device(hidden, norm_gain, head_weight, teacher_ids, teacher_probs, doc_ids, plan):
    seq_count, peers = lax.axis_size("seq"), lax.axis_size("vocab")
    vocab_local = head_weight.shape[1]
    shard = lax.axis_index("vocab")
    where = jnp.stack([shard // CORES, shard % CORES, shard * vocab_local]).astype(jnp.int32)
    turned = hidden.T
    width = turned.shape[1] // CHUNKS
    first, second = turned[:, :width], turned[:, width:]
    a0 = move(first, turn(1))
    b1 = move(second, turn(-1))
    b0 = move(first, turn(-1))
    weight = prepare(where, head_weight.T, norm_gain.reshape(-1, LANES))
    c0 = move(a0, turn(1))
    a1 = move(second, turn(1))
    c1 = move(b1, turn(-1))
    z0, z1 = move(first, SWAP), move(second, SWAP)
    a0s, b1s, b0s = move(a0, SWAP), move(b1, SWAP), move(b0, SWAP)
    c0s, c1s, a1s = move(c0, SWAP), move(c1, SWAP), move(a1, SWAP)
    near1 = near_head(where, weight, (second, z1, b1, b1s))
    near0 = near_head(where, weight, (first, z0, b0, b0s, a0, a0s))
    teacher = (teacher_ids, teacher_probs)
    earlier, mass = far_head(0, where, weight, *near0, *teacher, (c0, c0s), None, peers)
    (copies,) = far_head(1, where, weight, *near1, *teacher, (a1, a1s, c1, c1s), earlier, peers)

    came = lax.all_to_all(copies, "vocab", split_axis=0, concat_axis=0, tiled=True)
    message = losses(plan.T, came, mass, doc_ids.reshape(-1, BLOCK), seq_count)
    came = lax.all_to_all(message, "seq", split_axis=0, concat_axis=0, tiled=True)
    doc_loss, row_lse = finish(came)
    return (doc_loss.reshape(-1), row_lse.reshape(-1))


def solution(mesh):
    return jax.shard_map(
        per_device,
        mesh=mesh,
        in_specs=(
            P("seq", "vocab"),
            P(),
            P(None, "vocab"),
            P("seq", None),
            P("seq", None),
            P("seq"),
            P("seq", None),
        ),
        out_specs=(P(), P("seq")),
        check_vma=False,
    )
```

```python
import functools

import jax
import jax.numpy as jnp
from jax import lax
from jax.experimental import pallas as pl
from jax.experimental.pallas import tpu as pltpu
from jax.sharding import PartitionSpec as P


BLOCK = 128
WORK = 4
DOCS = 128
CHIPS = 4
CORES = 2
CHUNKS = 2
HOPS = (1, 0, 3, 2, 1)
SOFTCAP = 30.0
EPS = 1e-06
LANES = 128
MIB = 1 << 20


def on_diagonal():
    lane = lax.broadcasted_iota(jnp.int32, (BLOCK, LANES), 1)
    return lane == lax.broadcasted_iota(jnp.int32, (BLOCK, LANES), 0)


def as_row(column):
    return jnp.sum(jnp.where(on_diagonal(), column, 0.0), axis=0, keepdims=True)


def prepare_kernel(where_ref, weight_ref, gain_ref, out_ref):
    width = weight_ref.shape[1] // CHIPS
    tiles = width // LANES
    low = lax.broadcasted_iota(jnp.int32, (1, LANES), 1) < width // CORES % LANES
    for k, hop in enumerate(HOPS):
        chips = [lax.rem(where_ref[0] + h, CHIPS) for h in (hop, (CHIPS - hop) % CHIPS)]
        for t in range(tiles):

            def scaled(chip):
                gain = gain_ref[pl.ds(chip * tiles + t, 1), :]
                start = pl.multiple_of(chip * width + t * LANES, LANES)
                return weight_ref[:, pl.ds(start, LANES)].astype(jnp.float32) * gain

            if t == tiles // 2:
                part = jnp.where(low, scaled(chips[0]), scaled(chips[1]))
            else:
                part = scaled(chips[t > tiles // 2])
            to = k * width + t * LANES
            out_ref[:, to : to + LANES] = part.astype(jnp.bfloat16)


def prepare(where, weight, gain):
    vmem = pl.BlockSpec(memory_space=pltpu.VMEM)
    vocab, features = weight.shape
    return pl.pallas_call(
        prepare_kernel,
        out_shape=jax.ShapeDtypeStruct((vocab, features // CHIPS * len(HOPS)), jnp.bfloat16),
        in_specs=[pl.BlockSpec(memory_space=pltpu.SMEM), vmem, vmem],
        out_specs=vmem,
        compiler_params=pltpu.CompilerParams(vmem_limit_bytes=24 * MIB),
        cost_estimate=pl.CostEstimate(
            flops=500 * weight.size, bytes_accessed=4 * weight.size, transcendentals=0
        ),
        name="prepare",
    )(where, weight, gain)


def squares_of(pieces):
    total = 0.0
    for piece in pieces:
        for i in range(0, piece[0].shape[0], 16):
            wide = across(piece, i, 16).astype(jnp.float32)
            total = total + wide * wide
    return total


def across(piece, start, count):
    parts = [part[start : start + count, :] for part in piece]
    return parts[0] if len(parts) == 1 else jnp.concatenate(parts, axis=1)


def multiply(core, weight_ref, first, pieces):
    shard = pieces[0][0].shape[0]
    start, depth = first * CORES * shard, len(pieces) * shard
    rows = []
    for own, other in zip(pieces[::CORES], pieces[1::CORES]):
        own, other = across(own, 0, shard), across(other, 0, shard)
        rows += [jnp.where(core == 0, own, other), jnp.where(core == 0, other, own)]
    return jnp.dot(
        weight_ref[:, start : start + depth],
        jnp.concatenate(rows, axis=0),
        preferred_element_type=jnp.float32,
    )


def near_kernel(first, where_ref, weight_ref, *refs):
    pieces, (logits_ref, squares_ref) = [(p,) for p in refs[:-2]], refs[-2:]
    squares_ref[...] = squares_of(pieces)
    logits_ref[...] = multiply(where_ref[1], weight_ref, first, pieces)


def near_head(first, where, weight, pieces):
    vocab = weight.shape[0]
    shard, width = pieces[0].shape
    depth = shard * len(pieces)
    vmem = pl.BlockSpec(memory_space=pltpu.VMEM)
    return pl.pallas_call(
        functools.partial(near_kernel, first),
        out_shape=(
            jax.ShapeDtypeStruct((vocab, width), jnp.float32),
            jax.ShapeDtypeStruct((16, width), jnp.float32),
        ),
        in_specs=[pl.BlockSpec(memory_space=pltpu.SMEM)] + [vmem] * (1 + len(pieces)),
        out_specs=(vmem, vmem),
        compiler_params=pltpu.CompilerParams(vmem_limit_bytes=24 * MIB),
        cost_estimate=pl.CostEstimate(
            flops=2 * vocab * depth * width,
            bytes_accessed=2 * (vocab + width) * depth,
            transcendentals=0,
        ),
        name="near",
    )(where, weight, *pieces)


def far_kernel(chunk, first, features, counts, where_ref, weight_ref, near_ref, squares_ref, ids_ref, probs_ref, *refs):
    pieces = []
    for count in counts:
        pieces.append(refs[:count])
        refs = refs[count:]
    earlier = refs[0] if chunk else None
    outs, (logits_ref, scale_ref) = refs[bool(chunk) : -2], refs[-2:]
    vocab, width = near_ref.shape
    squares = squares_ref[...] + squares_of(pieces)
    mean = jnp.sum(squares, axis=0, keepdims=True) * (1.0 / features)
    scale = lax.rsqrt(mean + EPS) * (1.0 / SOFTCAP)
    scale_ref[...] = jnp.broadcast_to(scale, scale_ref.shape)
    logits_ref[...] = near_ref[...] + multiply(where_ref[1], weight_ref, first, pieces)

    blocks = width // BLOCK
    expsums, picks = [], []
    for q in range(blocks):
        lanes = slice(q * BLOCK, (q + 1) * BLOCK)
        scale = scale_ref[0:1, lanes]
        rows = slice((chunk * blocks + q) * BLOCK, (chunk * blocks + q + 1) * BLOCK)
        within = ids_ref[rows, :] - where_ref[2]
        tile, spot = within >> 7, within & (LANES - 1)
        sums = jnp.zeros((8, BLOCK), jnp.float32)
        turned = []
        for t in range(-(-vocab // LANES)):
            size = min(LANES, vocab - t * LANES)
            soft = jnp.tanh(logits_ref[t * LANES : t * LANES + size, lanes] * scale)
            power = jnp.exp(SOFTCAP * soft)
            sums = sums + jnp.sum(power.reshape(size // 8, 8, BLOCK), axis=0)
            if size < LANES:
                soft = jnp.concatenate([soft, jnp.zeros((LANES - size, BLOCK), jnp.float32)], axis=0)
            turned.append(soft.astype(jnp.bfloat16).T.astype(jnp.float32))
        chosen = []
        for g in range(0, BLOCK, 8):
            found = jnp.zeros((8, LANES), jnp.float32)
            for t, soft in enumerate(turned):
                part = jnp.take_along_axis(
                    soft[g : g + 8], spot[g : g + 8], axis=1, mode="promise_in_bounds"
                )
                found = jnp.where(tile[g : g + 8] == t, part, found)
            chosen.append(found)
        chosen = jnp.concatenate(chosen, axis=0)
        picked = SOFTCAP * jnp.sum(probs_ref[rows, :] * chosen, axis=1, keepdims=True)
        expsums.append(jnp.sum(sums, axis=0, keepdims=True))
        picks.append(as_row(picked))
    here = jnp.concatenate(expsums + picks, axis=0)
    if chunk == 0:
        stats_ref, mass_ref = outs
        stats_ref[...] = here
        for b in range(mass_ref.shape[0]):
            mass = jnp.sum(probs_ref[b * BLOCK : (b + 1) * BLOCK, :], axis=1, keepdims=True)
            mass_ref[b : b + 1, :] = as_row(mass)
    else:
        (copies_ref,) = outs
        before = earlier[...]
        for k in range(copies_ref.shape[0]):
            copies_ref[k, 0:blocks] = before[:blocks]
            copies_ref[k, blocks : 2 * blocks] = here[:blocks]
            copies_ref[k, 2 * blocks : 3 * blocks] = before[blocks:]
            copies_ref[k, 3 * blocks :] = here[blocks:]


def far_head(chunk, first, where, weight, near, squares, ids, probs, pieces, earlier, peers):
    vocab, width = near.shape
    counts = [len(piece) for piece in pieces]
    shard = pieces[0][0].shape[0]
    features = shard * CORES * CHIPS
    blocks = ids.shape[0] // BLOCK
    stat = lambda *shape: jax.ShapeDtypeStruct(shape, jnp.float32)
    if chunk == 0:
        out_shape = (stat(blocks, BLOCK), stat(blocks, BLOCK))
    else:
        out_shape = (stat(peers, 2 * blocks, BLOCK),)
    vmem = pl.BlockSpec(memory_space=pltpu.VMEM)
    parts = [part for piece in pieces for part in piece]
    operands = [weight, near, squares, ids, probs, *parts] + ([earlier] if chunk else [])
    depth = len(pieces) * shard
    return pl.pallas_call(
        functools.partial(far_kernel, chunk, first, features, counts),
        out_shape=out_shape,
        in_specs=[pl.BlockSpec(memory_space=pltpu.SMEM)] + [vmem] * len(operands),
        out_specs=(vmem,) * len(out_shape),
        scratch_shapes=[
            pltpu.VMEM((vocab, width), jnp.float32),
            pltpu.VMEM((8, width), jnp.float32),
        ],
        compiler_params=pltpu.CompilerParams(vmem_limit_bytes=24 * MIB),
        cost_estimate=pl.CostEstimate(
            flops=2 * 2 * vocab * depth * width,
            bytes_accessed=2 * (vocab + width) * depth + 8 * vocab * width,
            transcendentals=2 * vocab * width,
        ),
        name="far",
    )(where, *operands)


def losses_kernel(plan_ref, came_ref, mass_ref, docs_ref, message_ref):
    blocks = mass_ref.shape[0]
    sums = jnp.sum(came_ref[...], axis=0)
    expsum, picked = sums[:blocks], sums[blocks:]
    alive = docs_ref[...] >= 0
    lse = jnp.log(jnp.where(alive, expsum, 1.0))
    row_loss = jnp.where(alive, lse * mass_ref[...] - picked, 0.0)
    label = lax.broadcasted_iota(jnp.int32, (DOCS, LANES), 0)
    totals = jnp.zeros((DOCS, LANES), jnp.float32)
    counts = jnp.zeros((DOCS, LANES), jnp.float32)
    for b in range(blocks):
        member = label == docs_ref[b : b + 1, :]
        totals = totals + jnp.where(member, row_loss[b : b + 1, :], 0.0)
        counts = counts + jnp.where(member, 1.0, 0.0)
    totals = as_row(jnp.sum(totals, axis=1, keepdims=True))
    counts = as_row(jnp.sum(counts, axis=1, keepdims=True))
    peers = message_ref.shape[0]
    peer = lax.broadcasted_iota(jnp.int32, (peers, LANES), 0)
    routed = jnp.zeros((peers, LANES), jnp.float32)
    mark = jnp.zeros((peers, LANES), jnp.int32)
    for b in range(blocks):
        chosen = peer == plan_ref[0, b]
        routed = jnp.where(chosen, lse[b : b + 1, :], routed)
        mark = jnp.where(chosen, plan_ref[1, b] + 1, mark)
    message_ref[:, 0 * LANES : 1 * LANES] = routed
    message_ref[:, 1 * LANES : 2 * LANES] = jnp.broadcast_to(totals, (peers, LANES))
    message_ref[:, 2 * LANES : 3 * LANES] = jnp.broadcast_to(counts, (peers, LANES))
    message_ref[:, 3 * LANES : 4 * LANES] = mark.astype(jnp.float32)


def losses(plan, came, mass, docs, peers):
    vmem = pl.BlockSpec(memory_space=pltpu.VMEM)
    return pl.pallas_call(
        losses_kernel,
        out_shape=jax.ShapeDtypeStruct((peers, 4 * LANES), jnp.float32),
        in_specs=[pl.BlockSpec(memory_space=pltpu.SMEM), vmem, vmem, vmem],
        out_specs=vmem,
        compiler_params=pltpu.CompilerParams(vmem_limit_bytes=8 * MIB),
        name="losses",
    )(plan, came, mass, docs)


def finish_kernel(came_ref, doc_ref, lse_ref):
    mark = came_ref[:, 3 * LANES : 4 * LANES]
    came = came_ref[:, 0:LANES]
    for s in range(WORK):
        lse_ref[s : s + 1, :] = jnp.sum(
            jnp.where(mark == float(s + 1), came, 0.0), axis=0, keepdims=True
        )
    totals = jnp.sum(came_ref[:, LANES : 2 * LANES], axis=0, keepdims=True)
    counts = jnp.sum(came_ref[:, 2 * LANES : 3 * LANES], axis=0, keepdims=True)
    doc_ref[...] = totals / jnp.maximum(counts, 1.0)


def finish(came):
    vmem = pl.BlockSpec(memory_space=pltpu.VMEM)
    stat = lambda rows: jax.ShapeDtypeStruct((rows, LANES), jnp.float32)
    return pl.pallas_call(
        finish_kernel,
        out_shape=(stat(1), stat(WORK)),
        in_specs=[vmem],
        out_specs=(vmem, vmem),
        compiler_params=pltpu.CompilerParams(vmem_limit_bytes=8 * MIB),
        name="finish",
    )(came)


def turn(step):
    pairs = []
    for i in range(CORES * CHIPS):
        chip, core = i // CORES, i % CORES
        pairs.append((i, (chip + (step if core == 0 else -step)) % CHIPS * CORES + core))
    return pairs


SWAP = [(i, i ^ 1) for i in range(CORES * CHIPS)]


def move(x, pairs):
    return lax.ppermute(x, "vocab", pairs)


def per_device(hidden, norm_gain, head_weight, teacher_ids, teacher_probs, doc_ids, plan):
    seq_count, peers = lax.axis_size("seq"), lax.axis_size("vocab")
    vocab_local = head_weight.shape[1]
    shard = lax.axis_index("vocab")
    where = jnp.stack([shard // CORES, shard % CORES, shard * vocab_local]).astype(jnp.int32)
    turned = hidden.T
    width = turned.shape[1] // CHUNKS
    first, second = turned[:, :width], turned[:, width:]
    a0 = move(first, turn(1))
    b1 = move(second, turn(-1))
    b0 = move(first, turn(-1))
    weight = prepare(where, head_weight.T, norm_gain.reshape(-1, LANES))
    c0 = move(a0, turn(1))
    a1 = move(second, turn(1))
    c1 = move(b1, turn(-1))
    z0, z1 = move(first, SWAP), move(second, SWAP)
    a0s, b1s, b0s = move(a0, SWAP), move(b1, SWAP), move(b0, SWAP)
    c0s, c1s, a1s = move(c0, SWAP), move(c1, SWAP), move(a1, SWAP)
    near1 = near_head(0, where, weight, (b1, b1s, second, z1))
    near0 = near_head(1, where, weight, (first, z0, a0, a0s))
    teacher = (teacher_ids, teacher_probs)
    earlier, mass = far_head(
        0, 3, where, weight, *near0, *teacher, ((c0,), (c0s,), (b0,), (b0s,)), None, peers
    )
    late = ((a1,), (a1s,), (c1,), (c1s,))
    (copies,) = far_head(
        1, 2, where, weight, *near1, *teacher, late, earlier, peers
    )

    came = lax.all_to_all(copies, "vocab", split_axis=0, concat_axis=0, tiled=True)
    message = losses(plan.T, came, mass, doc_ids.reshape(-1, BLOCK), seq_count)
    came = lax.all_to_all(message, "seq", split_axis=0, concat_axis=0, tiled=True)
    doc_loss, row_lse = finish(came)
    return (doc_loss.reshape(-1), row_lse.reshape(-1))


def solution(mesh):
    return jax.shard_map(
        per_device,
        mesh=mesh,
        in_specs=(
            P("seq", "vocab"),
            P(),
            P(None, "vocab"),
            P("seq", None),
            P("seq", None),
            P("seq"),
            P("seq", None),
        ),
        out_specs=(P(), P("seq")),
        check_vma=False,
    )
```

```python
import functools

import jax
import jax.numpy as jnp
from jax import lax
from jax.experimental import pallas as pl
from jax.experimental.pallas import tpu as pltpu
from jax.sharding import PartitionSpec as P


BLOCK = 128
WORK = 4
DOCS = 128
CHIPS = 4
CORES = 2
CHUNKS = 2
HOPS = (1, 0, 3, 2, 1)
SOFTCAP = 30.0
EPS = 1e-06
LANES = 128
MIB = 1 << 20


def on_diagonal():
    lane = lax.broadcasted_iota(jnp.int32, (BLOCK, LANES), 1)
    return lane == lax.broadcasted_iota(jnp.int32, (BLOCK, LANES), 0)


def as_row(column):
    return jnp.sum(jnp.where(on_diagonal(), column, 0.0), axis=0, keepdims=True)


def prepare_kernel(where_ref, weight_ref, gain_ref, out_ref):
    width = weight_ref.shape[1] // CHIPS
    tiles = width // LANES
    low = lax.broadcasted_iota(jnp.int32, (1, LANES), 1) < width // CORES % LANES
    for k, hop in enumerate(HOPS):
        chips = [lax.rem(where_ref[0] + h, CHIPS) for h in (hop, (CHIPS - hop) % CHIPS)]
        for t in range(tiles):

            def scaled(chip):
                gain = gain_ref[pl.ds(chip * tiles + t, 1), :]
                start = pl.multiple_of(chip * width + t * LANES, LANES)
                return weight_ref[:, pl.ds(start, LANES)].astype(jnp.float32) * gain

            if t == tiles // 2:
                part = jnp.where(low, scaled(chips[0]), scaled(chips[1]))
            else:
                part = scaled(chips[t > tiles // 2])
            to = k * width + t * LANES
            out_ref[:, to : to + LANES] = part.astype(jnp.bfloat16)


def prepare(where, weight, gain):
    vmem = pl.BlockSpec(memory_space=pltpu.VMEM)
    vocab, features = weight.shape
    return pl.pallas_call(
        prepare_kernel,
        out_shape=jax.ShapeDtypeStruct((vocab, features // CHIPS * len(HOPS)), jnp.bfloat16),
        in_specs=[pl.BlockSpec(memory_space=pltpu.SMEM), vmem, vmem],
        out_specs=vmem,
        compiler_params=pltpu.CompilerParams(vmem_limit_bytes=24 * MIB),
        cost_estimate=pl.CostEstimate(
            flops=500 * weight.size, bytes_accessed=4 * weight.size, transcendentals=0
        ),
        name="prepare",
    )(where, weight, gain)


def squares_of(pieces):
    total = 0.0
    for piece in pieces:
        for i in range(0, piece.shape[0], 16):
            wide = piece[i : i + 16, :].astype(jnp.float32)
            total = total + wide * wide
    return total


def multiply(core, weight_ref, first, pieces):
    shard = pieces[0].shape[0]
    start, depth = first * CORES * shard, len(pieces) * shard
    rows = []
    for own, other in zip(pieces[::CORES], pieces[1::CORES]):
        own, other = own[...], other[...]
        rows += [jnp.where(core == 0, own, other), jnp.where(core == 0, other, own)]
    return jnp.dot(
        weight_ref[:, start : start + depth],
        jnp.concatenate(rows, axis=0),
        preferred_element_type=jnp.float32,
    )


def multiply_side(core, weight_ref, first, pieces):
    shard, width = pieces[0].shape
    wide = -(-shard // LANES) * LANES
    rest = jnp.zeros((wide - shard, width), jnp.bfloat16)
    rows, columns = [], []
    for k, piece in enumerate(pieces):
        start = (first + k) * CORES * shard + core * (CORES * shard - wide)
        columns.append(weight_ref[:, pl.ds(pl.multiple_of(start, LANES), wide)])
        low = jnp.concatenate([piece[...], rest], axis=0)
        high = jnp.concatenate([rest, piece[...]], axis=0)
        rows.append(jnp.where(core == 0, low, high))
    return jnp.dot(
        jnp.concatenate(columns, axis=1),
        jnp.concatenate(rows, axis=0),
        preferred_element_type=jnp.float32,
    )


def middle_kernel(first, where_ref, weight_ref, near_ref, near_squares_ref, *refs):
    pieces, (logits_ref, squares_ref) = refs[:-2], refs[-2:]
    squares_ref[...] = near_squares_ref[...] + squares_of(pieces)
    logits_ref[...] = near_ref[...] + multiply_side(where_ref[1], weight_ref, first, pieces)


def middle(first, where, weight, near, squares, pieces):
    vmem = pl.BlockSpec(memory_space=pltpu.VMEM)
    vocab, width = near.shape
    depth = len(pieces) * pieces[0].shape[0]
    return pl.pallas_call(
        functools.partial(middle_kernel, first),
        out_shape=tuple(jax.ShapeDtypeStruct(a.shape, a.dtype) for a in (near, squares)),
        in_specs=[pl.BlockSpec(memory_space=pltpu.SMEM)] + [vmem] * (3 + len(pieces)),
        out_specs=(vmem, vmem),
        compiler_params=pltpu.CompilerParams(vmem_limit_bytes=24 * MIB),
        cost_estimate=pl.CostEstimate(
            flops=2 * vocab * depth * width,
            bytes_accessed=2 * (vocab + width) * depth + 8 * vocab * width,
            transcendentals=0,
        ),
        name="middle",
    )(where, weight, near, squares, *pieces)


def near_kernel(first, where_ref, weight_ref, *refs):
    pieces, (logits_ref, squares_ref) = refs[:-2], refs[-2:]
    squares_ref[...] = squares_of(pieces)
    logits_ref[...] = multiply(where_ref[1], weight_ref, first, pieces)


def near_head(first, where, weight, pieces):
    vocab = weight.shape[0]
    shard, width = pieces[0].shape
    depth = shard * len(pieces)
    vmem = pl.BlockSpec(memory_space=pltpu.VMEM)
    return pl.pallas_call(
        functools.partial(near_kernel, first),
        out_shape=(
            jax.ShapeDtypeStruct((vocab, width), jnp.float32),
            jax.ShapeDtypeStruct((16, width), jnp.float32),
        ),
        in_specs=[pl.BlockSpec(memory_space=pltpu.SMEM)] + [vmem] * (1 + len(pieces)),
        out_specs=(vmem, vmem),
        compiler_params=pltpu.CompilerParams(vmem_limit_bytes=24 * MIB),
        cost_estimate=pl.CostEstimate(
            flops=2 * vocab * depth * width,
            bytes_accessed=2 * (vocab + width) * depth,
            transcendentals=0,
        ),
        name="near",
    )(where, weight, *pieces)


def far_kernel(chunk, first, features, count, where_ref, weight_ref, near_ref, squares_ref, ids_ref, probs_ref, *refs):
    pieces, refs = refs[:count], refs[count:]
    earlier = refs[0] if chunk else None
    outs, (logits_ref, scale_ref) = refs[bool(chunk) : -2], refs[-2:]
    vocab, width = near_ref.shape
    squares = squares_ref[...] + squares_of(pieces)
    mean = jnp.sum(squares, axis=0, keepdims=True) * (1.0 / features)
    scale = lax.rsqrt(mean + EPS) * (1.0 / SOFTCAP)
    scale_ref[...] = jnp.broadcast_to(scale, scale_ref.shape)
    if chunk == 0:
        late = multiply(where_ref[1], weight_ref, first, pieces)
    else:
        late = multiply_side(1 - where_ref[1], weight_ref, first, pieces)
    logits_ref[...] = near_ref[...] + late

    blocks = width // BLOCK
    expsums, picks = [], []
    for q in range(blocks):
        lanes = slice(q * BLOCK, (q + 1) * BLOCK)
        scale = scale_ref[0:1, lanes]
        rows = slice((chunk * blocks + q) * BLOCK, (chunk * blocks + q + 1) * BLOCK)
        within = ids_ref[rows, :] - where_ref[2]
        tile, spot = within >> 7, within & (LANES - 1)
        sums = jnp.zeros((8, BLOCK), jnp.float32)
        turned = []
        for t in range(-(-vocab // LANES)):
            size = min(LANES, vocab - t * LANES)
            soft = jnp.tanh(logits_ref[t * LANES : t * LANES + size, lanes] * scale)
            power = jnp.exp(SOFTCAP * soft)
            sums = sums + jnp.sum(power.reshape(size // 8, 8, BLOCK), axis=0)
            if size < LANES:
                soft = jnp.concatenate([soft, jnp.zeros((LANES - size, BLOCK), jnp.float32)], axis=0)
            turned.append(soft.astype(jnp.bfloat16).T.astype(jnp.float32))
        chosen = []
        for g in range(0, BLOCK, 8):
            found = jnp.zeros((8, LANES), jnp.float32)
            for t, soft in enumerate(turned):
                part = jnp.take_along_axis(
                    soft[g : g + 8], spot[g : g + 8], axis=1, mode="promise_in_bounds"
                )
                found = jnp.where(tile[g : g + 8] == t, part, found)
            chosen.append(found)
        chosen = jnp.concatenate(chosen, axis=0)
        picked = SOFTCAP * jnp.sum(probs_ref[rows, :] * chosen, axis=1, keepdims=True)
        expsums.append(jnp.sum(sums, axis=0, keepdims=True))
        picks.append(as_row(picked))
    here = jnp.concatenate(expsums + picks, axis=0)
    if chunk == 0:
        stats_ref, mass_ref = outs
        stats_ref[...] = here
        for b in range(mass_ref.shape[0]):
            mass = jnp.sum(probs_ref[b * BLOCK : (b + 1) * BLOCK, :], axis=1, keepdims=True)
            mass_ref[b : b + 1, :] = as_row(mass)
    else:
        (copies_ref,) = outs
        before = earlier[...]
        for k in range(copies_ref.shape[0]):
            copies_ref[k, 0:blocks] = before[:blocks]
            copies_ref[k, blocks : 2 * blocks] = here[:blocks]
            copies_ref[k, 2 * blocks : 3 * blocks] = before[blocks:]
            copies_ref[k, 3 * blocks :] = here[blocks:]


def far_head(chunk, first, where, weight, near, squares, ids, probs, pieces, earlier, peers):
    vocab, width = near.shape
    shard = pieces[0].shape[0]
    features = shard * CORES * CHIPS
    blocks = ids.shape[0] // BLOCK
    stat = lambda *shape: jax.ShapeDtypeStruct(shape, jnp.float32)
    if chunk == 0:
        out_shape = (stat(blocks, BLOCK), stat(blocks, BLOCK))
    else:
        out_shape = (stat(peers, 2 * blocks, BLOCK),)
    vmem = pl.BlockSpec(memory_space=pltpu.VMEM)
    operands = [weight, near, squares, ids, probs, *pieces] + ([earlier] if chunk else [])
    depth = len(pieces) * shard
    return pl.pallas_call(
        functools.partial(far_kernel, chunk, first, features, len(pieces)),
        out_shape=out_shape,
        in_specs=[pl.BlockSpec(memory_space=pltpu.SMEM)] + [vmem] * len(operands),
        out_specs=(vmem,) * len(out_shape),
        scratch_shapes=[
            pltpu.VMEM((vocab, width), jnp.float32),
            pltpu.VMEM((8, width), jnp.float32),
        ],
        compiler_params=pltpu.CompilerParams(vmem_limit_bytes=24 * MIB),
        cost_estimate=pl.CostEstimate(
            flops=2 * 2 * vocab * depth * width,
            bytes_accessed=2 * (vocab + width) * depth + 8 * vocab * width,
            transcendentals=2 * vocab * width,
        ),
        name="far",
    )(where, *operands)


def losses_kernel(plan_ref, came_ref, mass_ref, docs_ref, message_ref):
    blocks = mass_ref.shape[0]
    sums = jnp.sum(came_ref[...], axis=0)
    expsum, picked = sums[:blocks], sums[blocks:]
    alive = docs_ref[...] >= 0
    lse = jnp.log(jnp.where(alive, expsum, 1.0))
    row_loss = jnp.where(alive, lse * mass_ref[...] - picked, 0.0)
    label = lax.broadcasted_iota(jnp.int32, (DOCS, LANES), 0)
    totals = jnp.zeros((DOCS, LANES), jnp.float32)
    counts = jnp.zeros((DOCS, LANES), jnp.float32)
    for b in range(blocks):
        member = label == docs_ref[b : b + 1, :]
        totals = totals + jnp.where(member, row_loss[b : b + 1, :], 0.0)
        counts = counts + jnp.where(member, 1.0, 0.0)
    totals = as_row(jnp.sum(totals, axis=1, keepdims=True))
    counts = as_row(jnp.sum(counts, axis=1, keepdims=True))
    peers = message_ref.shape[0]
    peer = lax.broadcasted_iota(jnp.int32, (peers, LANES), 0)
    routed = jnp.zeros((peers, LANES), jnp.float32)
    mark = jnp.zeros((peers, LANES), jnp.int32)
    for b in range(blocks):
        chosen = peer == plan_ref[0, b]
        routed = jnp.where(chosen, lse[b : b + 1, :], routed)
        mark = jnp.where(chosen, plan_ref[1, b] + 1, mark)
    message_ref[:, 0 * LANES : 1 * LANES] = routed
    message_ref[:, 1 * LANES : 2 * LANES] = jnp.broadcast_to(totals, (peers, LANES))
    message_ref[:, 2 * LANES : 3 * LANES] = jnp.broadcast_to(counts, (peers, LANES))
    message_ref[:, 3 * LANES : 4 * LANES] = mark.astype(jnp.float32)


def losses(plan, came, mass, docs, peers):
    vmem = pl.BlockSpec(memory_space=pltpu.VMEM)
    return pl.pallas_call(
        losses_kernel,
        out_shape=jax.ShapeDtypeStruct((peers, 4 * LANES), jnp.float32),
        in_specs=[pl.BlockSpec(memory_space=pltpu.SMEM), vmem, vmem, vmem],
        out_specs=vmem,
        compiler_params=pltpu.CompilerParams(vmem_limit_bytes=8 * MIB),
        name="losses",
    )(plan, came, mass, docs)


def finish_kernel(came_ref, doc_ref, lse_ref):
    mark = came_ref[:, 3 * LANES : 4 * LANES]
    came = came_ref[:, 0:LANES]
    for s in range(WORK):
        lse_ref[s : s + 1, :] = jnp.sum(
            jnp.where(mark == float(s + 1), came, 0.0), axis=0, keepdims=True
        )
    totals = jnp.sum(came_ref[:, LANES : 2 * LANES], axis=0, keepdims=True)
    counts = jnp.sum(came_ref[:, 2 * LANES : 3 * LANES], axis=0, keepdims=True)
    doc_ref[...] = totals / jnp.maximum(counts, 1.0)


def finish(came):
    vmem = pl.BlockSpec(memory_space=pltpu.VMEM)
    stat = lambda rows: jax.ShapeDtypeStruct((rows, LANES), jnp.float32)
    return pl.pallas_call(
        finish_kernel,
        out_shape=(stat(1), stat(WORK)),
        in_specs=[vmem],
        out_specs=(vmem, vmem),
        compiler_params=pltpu.CompilerParams(vmem_limit_bytes=8 * MIB),
        name="finish",
    )(came)


def turn(step):
    pairs = []
    for i in range(CORES * CHIPS):
        chip, core = i // CORES, i % CORES
        pairs.append((i, (chip + (step if core == 0 else -step)) % CHIPS * CORES + core))
    return pairs


SWAP = [(i, i ^ 1) for i in range(CORES * CHIPS)]


def move(x, pairs):
    return lax.ppermute(x, "vocab", pairs)


def per_device(hidden, norm_gain, head_weight, teacher_ids, teacher_probs, doc_ids, plan):
    seq_count, peers = lax.axis_size("seq"), lax.axis_size("vocab")
    vocab_local = head_weight.shape[1]
    shard = lax.axis_index("vocab")
    where = jnp.stack([shard // CORES, shard % CORES, shard * vocab_local]).astype(jnp.int32)
    turned = hidden.T
    width = turned.shape[1] // CHUNKS
    first, second = turned[:, :width], turned[:, width:]
    a0 = move(first, turn(1))
    b1 = move(second, turn(-1))
    b0 = move(first, turn(-1))
    weight = prepare(where, head_weight.T, norm_gain.reshape(-1, LANES))
    c0 = move(a0, turn(1))
    a1 = move(second, turn(1))
    c1 = move(b1, turn(-1))
    z0, z1 = move(first, SWAP), move(second, SWAP)
    a0s, b1s, b0s = move(a0, SWAP), move(b1, SWAP), move(b0, SWAP)
    c0s, c1s, a1s = move(c0, SWAP), move(c1, SWAP), move(a1, SWAP)
    near1 = near_head(0, where, weight, (b1, b1s, second, z1))
    near0 = near_head(1, where, weight, (first, z0, a0, a0s))
    teacher = (teacher_ids, teacher_probs)
    earlier, mass = far_head(0, 3, where, weight, *near0, *teacher, (c0, c0s, b0, b0s), None, peers)
    near1 = middle(2, where, weight, *near1, (a1, c1))
    late = (a1s, c1s)
    (copies,) = far_head(
        1, 2, where, weight, *near1, *teacher, late, earlier, peers
    )

    came = lax.all_to_all(copies, "vocab", split_axis=0, concat_axis=0, tiled=True)
    message = losses(plan.T, came, mass, doc_ids.reshape(-1, BLOCK), seq_count)
    came = lax.all_to_all(message, "seq", split_axis=0, concat_axis=0, tiled=True)
    doc_loss, row_lse = finish(came)
    return (doc_loss.reshape(-1), row_lse.reshape(-1))


def solution(mesh):
    return jax.shard_map(
        per_device,
        mesh=mesh,
        in_specs=(
            P("seq", "vocab"),
            P(),
            P(None, "vocab"),
            P("seq", None),
            P("seq", None),
            P("seq"),
            P("seq", None),
        ),
        out_specs=(P(), P("seq")),
        check_vma=False,
    )
```

```python
import functools

import jax
import jax.numpy as jnp
from jax import lax
from jax.experimental import pallas as pl
from jax.experimental.pallas import tpu as pltpu
from jax.sharding import PartitionSpec as P


BLOCK = 128
WORK = 4
DOCS = 128
CHIPS = 4
CORES = 2
CHUNKS = 2
HOPS = (1, 0, 3, 2, 1)
SOFTCAP = 30.0
EPS = 1e-06
LANES = 128
BAND = 256
MIB = 1 << 20


def on_diagonal():
    lane = lax.broadcasted_iota(jnp.int32, (BLOCK, LANES), 1)
    return lane == lax.broadcasted_iota(jnp.int32, (BLOCK, LANES), 0)


def as_row(column):
    return jnp.sum(jnp.where(on_diagonal(), column, 0.0), axis=0, keepdims=True)


def prepare_kernel(where_ref, weight_ref, gain_ref, out_ref):
    width = weight_ref.shape[1] // CHIPS
    tiles = width // LANES
    low = lax.broadcasted_iota(jnp.int32, (1, LANES), 1) < width // CORES % LANES
    for k, hop in enumerate(HOPS):
        chips = [lax.rem(where_ref[0] + h, CHIPS) for h in (hop, (CHIPS - hop) % CHIPS)]
        for t in range(tiles):

            def scaled(chip):
                gain = gain_ref[pl.ds(chip * tiles + t, 1), :]
                start = pl.multiple_of(chip * width + t * LANES, LANES)
                return weight_ref[:, pl.ds(start, LANES)].astype(jnp.float32) * gain

            if t == tiles // 2:
                part = jnp.where(low, scaled(chips[0]), scaled(chips[1]))
            else:
                part = scaled(chips[t > tiles // 2])
            to = k * width + t * LANES
            out_ref[:, to : to + LANES] = part.astype(jnp.bfloat16)


def prepare(where, weight, gain):
    vmem = pl.BlockSpec(memory_space=pltpu.VMEM)
    vocab, features = weight.shape
    return pl.pallas_call(
        prepare_kernel,
        out_shape=jax.ShapeDtypeStruct((vocab, features // CHIPS * len(HOPS)), jnp.bfloat16),
        in_specs=[pl.BlockSpec(memory_space=pltpu.SMEM), vmem, vmem],
        out_specs=vmem,
        compiler_params=pltpu.CompilerParams(vmem_limit_bytes=24 * MIB),
        cost_estimate=pl.CostEstimate(
            flops=500 * weight.size, bytes_accessed=4 * weight.size, transcendentals=0
        ),
        name="prepare",
    )(where, weight, gain)


def squares_of(pieces):
    total = 0.0
    for piece in pieces:
        for i in range(0, piece.shape[0], 16):
            wide = piece[i : i + 16, :].astype(jnp.float32)
            total = total + wide * wide
    return total


def pair_rows(core, pieces):
    rows = []
    for own, other in zip(pieces[::CORES], pieces[1::CORES]):
        own, other = own[...], other[...]
        rows += [jnp.where(core == 0, own, other), jnp.where(core == 0, other, own)]
    return jnp.concatenate(rows, axis=0)


def pair_columns(weight_ref, first, pieces, band):
    shard = pieces[0].shape[0]
    start = first * CORES * shard
    return weight_ref[band, start : start + len(pieces) * shard]


def multiply(core, weight_ref, first, pieces):
    return jnp.dot(
        pair_columns(weight_ref, first, pieces, slice(None)),
        pair_rows(core, pieces),
        preferred_element_type=jnp.float32,
    )


def side_rows(core, pieces):
    shard, width = pieces[0].shape
    rest = jnp.zeros((-shard % LANES, width), jnp.bfloat16)
    rows = []
    for piece in pieces:
        low = jnp.concatenate([piece[...], rest], axis=0)
        high = jnp.concatenate([rest, piece[...]], axis=0)
        rows.append(jnp.where(core == 0, low, high))
    return jnp.concatenate(rows, axis=0)


def side_columns(core, weight_ref, first, pieces, band):
    shard = pieces[0].shape[0]
    wide = shard + -shard % LANES
    columns = []
    for k in range(len(pieces)):
        start = (first + k) * CORES * shard + core * (CORES * shard - wide)
        columns.append(weight_ref[band, pl.ds(pl.multiple_of(start, LANES), wide)])
    return jnp.concatenate(columns, axis=1)


def middle_kernel(first, where_ref, weight_ref, near_ref, near_squares_ref, *refs):
    pieces, (logits_ref, squares_ref) = refs[:-2], refs[-2:]
    squares_ref[...] = near_squares_ref[...] + squares_of(pieces)
    logits_ref[...] = near_ref[...] + jnp.dot(
        side_columns(where_ref[1], weight_ref, first, pieces, slice(None)),
        side_rows(where_ref[1], pieces),
        preferred_element_type=jnp.float32,
    )


def middle(first, where, weight, near, squares, pieces):
    vmem = pl.BlockSpec(memory_space=pltpu.VMEM)
    vocab, width = near.shape
    depth = len(pieces) * pieces[0].shape[0]
    return pl.pallas_call(
        functools.partial(middle_kernel, first),
        out_shape=tuple(jax.ShapeDtypeStruct(a.shape, a.dtype) for a in (near, squares)),
        in_specs=[pl.BlockSpec(memory_space=pltpu.SMEM)] + [vmem] * (3 + len(pieces)),
        out_specs=(vmem, vmem),
        compiler_params=pltpu.CompilerParams(vmem_limit_bytes=24 * MIB),
        cost_estimate=pl.CostEstimate(
            flops=2 * vocab * depth * width,
            bytes_accessed=2 * (vocab + width) * depth + 8 * vocab * width,
            transcendentals=0,
        ),
        name="middle",
    )(where, weight, near, squares, *pieces)


def near_kernel(first, where_ref, weight_ref, *refs):
    pieces, (logits_ref, squares_ref) = refs[:-2], refs[-2:]
    squares_ref[...] = squares_of(pieces)
    logits_ref[...] = multiply(where_ref[1], weight_ref, first, pieces)


def near_head(first, where, weight, pieces):
    vocab = weight.shape[0]
    shard, width = pieces[0].shape
    depth = shard * len(pieces)
    vmem = pl.BlockSpec(memory_space=pltpu.VMEM)
    return pl.pallas_call(
        functools.partial(near_kernel, first),
        out_shape=(
            jax.ShapeDtypeStruct((vocab, width), jnp.float32),
            jax.ShapeDtypeStruct((16, width), jnp.float32),
        ),
        in_specs=[pl.BlockSpec(memory_space=pltpu.SMEM)] + [vmem] * (1 + len(pieces)),
        out_specs=(vmem, vmem),
        compiler_params=pltpu.CompilerParams(vmem_limit_bytes=24 * MIB),
        cost_estimate=pl.CostEstimate(
            flops=2 * vocab * depth * width,
            bytes_accessed=2 * (vocab + width) * depth,
            transcendentals=0,
        ),
        name="near",
    )(where, weight, *pieces)


def far_kernel(chunk, first, features, count, where_ref, weight_ref, near_ref, squares_ref, ids_ref, probs_ref, *refs):
    pieces, refs = refs[:count], refs[count:]
    earlier = refs[0] if chunk else None
    outs, soft_ref = refs[bool(chunk) : -1], refs[-1]
    vocab, width = near_ref.shape
    squares = squares_ref[...] + squares_of(pieces)
    mean = jnp.sum(squares, axis=0, keepdims=True) * (1.0 / features)
    scale = lax.rsqrt(mean + EPS) * (1.0 / SOFTCAP)
    core = where_ref[1] if chunk == 0 else 1 - where_ref[1]
    rows = pair_rows(core, pieces) if chunk == 0 else side_rows(core, pieces)
    for start in range(0, vocab, BAND):
        band = slice(start, min(start + BAND, vocab))
        if chunk == 0:
            columns = pair_columns(weight_ref, first, pieces, band)
        else:
            columns = side_columns(core, weight_ref, first, pieces, band)
        late = jnp.dot(columns, rows, preferred_element_type=jnp.float32)
        soft_ref[band, :] = jnp.tanh((near_ref[band, :] + late) * scale)

    blocks = width // BLOCK
    expsums, picks = [], []
    for q in range(blocks):
        lanes = slice(q * BLOCK, (q + 1) * BLOCK)
        rows = slice((chunk * blocks + q) * BLOCK, (chunk * blocks + q + 1) * BLOCK)
        within = ids_ref[rows, :] - where_ref[2]
        tile, spot = within >> 7, within & (LANES - 1)
        sums = jnp.zeros((8, BLOCK), jnp.float32)
        turned = []
        for t in range(-(-vocab // LANES)):
            size = min(LANES, vocab - t * LANES)
            soft = soft_ref[t * LANES : t * LANES + size, lanes]
            power = jnp.exp(SOFTCAP * soft)
            sums = sums + jnp.sum(power.reshape(size // 8, 8, BLOCK), axis=0)
            if size < LANES:
                soft = jnp.concatenate([soft, jnp.zeros((LANES - size, BLOCK), jnp.float32)], axis=0)
            turned.append(soft.astype(jnp.bfloat16).T.astype(jnp.float32))
        chosen = []
        for g in range(0, BLOCK, 8):
            found = jnp.zeros((8, LANES), jnp.float32)
            for t, soft in enumerate(turned):
                part = jnp.take_along_axis(
                    soft[g : g + 8], spot[g : g + 8], axis=1, mode="promise_in_bounds"
                )
                found = jnp.where(tile[g : g + 8] == t, part, found)
            chosen.append(found)
        chosen = jnp.concatenate(chosen, axis=0)
        picked = SOFTCAP * jnp.sum(probs_ref[rows, :] * chosen, axis=1, keepdims=True)
        expsums.append(jnp.sum(sums, axis=0, keepdims=True))
        picks.append(as_row(picked))
    here = jnp.concatenate(expsums + picks, axis=0)
    if chunk == 0:
        stats_ref, mass_ref = outs
        stats_ref[...] = here
        for b in range(mass_ref.shape[0]):
            mass = jnp.sum(probs_ref[b * BLOCK : (b + 1) * BLOCK, :], axis=1, keepdims=True)
            mass_ref[b : b + 1, :] = as_row(mass)
    else:
        (copies_ref,) = outs
        before = earlier[...]
        for k in range(copies_ref.shape[0]):
            copies_ref[k, 0:blocks] = before[:blocks]
            copies_ref[k, blocks : 2 * blocks] = here[:blocks]
            copies_ref[k, 2 * blocks : 3 * blocks] = before[blocks:]
            copies_ref[k, 3 * blocks :] = here[blocks:]


def far_head(chunk, first, where, weight, near, squares, ids, probs, pieces, earlier, peers):
    vocab, width = near.shape
    shard = pieces[0].shape[0]
    features = shard * CORES * CHIPS
    blocks = ids.shape[0] // BLOCK
    stat = lambda *shape: jax.ShapeDtypeStruct(shape, jnp.float32)
    if chunk == 0:
        out_shape = (stat(blocks, BLOCK), stat(blocks, BLOCK))
    else:
        out_shape = (stat(peers, 2 * blocks, BLOCK),)
    vmem = pl.BlockSpec(memory_space=pltpu.VMEM)
    operands = [weight, near, squares, ids, probs, *pieces] + ([earlier] if chunk else [])
    depth = len(pieces) * shard
    return pl.pallas_call(
        functools.partial(far_kernel, chunk, first, features, len(pieces)),
        out_shape=out_shape,
        in_specs=[pl.BlockSpec(memory_space=pltpu.SMEM)] + [vmem] * len(operands),
        out_specs=(vmem,) * len(out_shape),
        scratch_shapes=[pltpu.VMEM((vocab, width), jnp.float32)],
        compiler_params=pltpu.CompilerParams(vmem_limit_bytes=24 * MIB),
        cost_estimate=pl.CostEstimate(
            flops=2 * 2 * vocab * depth * width,
            bytes_accessed=2 * (vocab + width) * depth + 8 * vocab * width,
            transcendentals=2 * vocab * width,
        ),
        name="far",
    )(where, *operands)


def losses_kernel(plan_ref, came_ref, mass_ref, docs_ref, message_ref):
    blocks = mass_ref.shape[0]
    sums = jnp.sum(came_ref[...], axis=0)
    expsum, picked = sums[:blocks], sums[blocks:]
    alive = docs_ref[...] >= 0
    lse = jnp.log(jnp.where(alive, expsum, 1.0))
    row_loss = jnp.where(alive, lse * mass_ref[...] - picked, 0.0)
    label = lax.broadcasted_iota(jnp.int32, (DOCS, LANES), 0)
    totals = jnp.zeros((DOCS, LANES), jnp.float32)
    counts = jnp.zeros((DOCS, LANES), jnp.float32)
    for b in range(blocks):
        member = label == docs_ref[b : b + 1, :]
        totals = totals + jnp.where(member, row_loss[b : b + 1, :], 0.0)
        counts = counts + jnp.where(member, 1.0, 0.0)
    totals = as_row(jnp.sum(totals, axis=1, keepdims=True))
    counts = as_row(jnp.sum(counts, axis=1, keepdims=True))
    peers = message_ref.shape[0]
    peer = lax.broadcasted_iota(jnp.int32, (peers, LANES), 0)
    routed = jnp.zeros((peers, LANES), jnp.float32)
    mark = jnp.zeros((peers, LANES), jnp.int32)
    for b in range(blocks):
        chosen = peer == plan_ref[0, b]
        routed = jnp.where(chosen, lse[b : b + 1, :], routed)
        mark = jnp.where(chosen, plan_ref[1, b] + 1, mark)
    message_ref[:, 0 * LANES : 1 * LANES] = routed
    message_ref[:, 1 * LANES : 2 * LANES] = jnp.broadcast_to(totals, (peers, LANES))
    message_ref[:, 2 * LANES : 3 * LANES] = jnp.broadcast_to(counts, (peers, LANES))
    message_ref[:, 3 * LANES : 4 * LANES] = mark.astype(jnp.float32)


def losses(plan, came, mass, docs, peers):
    vmem = pl.BlockSpec(memory_space=pltpu.VMEM)
    return pl.pallas_call(
        losses_kernel,
        out_shape=jax.ShapeDtypeStruct((peers, 4 * LANES), jnp.float32),
        in_specs=[pl.BlockSpec(memory_space=pltpu.SMEM), vmem, vmem, vmem],
        out_specs=vmem,
        compiler_params=pltpu.CompilerParams(vmem_limit_bytes=8 * MIB),
        name="losses",
    )(plan, came, mass, docs)


def finish_kernel(came_ref, doc_ref, lse_ref):
    mark = came_ref[:, 3 * LANES : 4 * LANES]
    came = came_ref[:, 0:LANES]
    for s in range(WORK):
        lse_ref[s : s + 1, :] = jnp.sum(
            jnp.where(mark == float(s + 1), came, 0.0), axis=0, keepdims=True
        )
    totals = jnp.sum(came_ref[:, LANES : 2 * LANES], axis=0, keepdims=True)
    counts = jnp.sum(came_ref[:, 2 * LANES : 3 * LANES], axis=0, keepdims=True)
    doc_ref[...] = totals / jnp.maximum(counts, 1.0)


def finish(came):
    vmem = pl.BlockSpec(memory_space=pltpu.VMEM)
    stat = lambda rows: jax.ShapeDtypeStruct((rows, LANES), jnp.float32)
    return pl.pallas_call(
        finish_kernel,
        out_shape=(stat(1), stat(WORK)),
        in_specs=[vmem],
        out_specs=(vmem, vmem),
        compiler_params=pltpu.CompilerParams(vmem_limit_bytes=8 * MIB),
        name="finish",
    )(came)


def turn(step):
    pairs = []
    for i in range(CORES * CHIPS):
        chip, core = i // CORES, i % CORES
        pairs.append((i, (chip + (step if core == 0 else -step)) % CHIPS * CORES + core))
    return pairs


SWAP = [(i, i ^ 1) for i in range(CORES * CHIPS)]


def move(x, pairs):
    return lax.ppermute(x, "vocab", pairs)


def per_device(hidden, norm_gain, head_weight, teacher_ids, teacher_probs, doc_ids, plan):
    seq_count, peers = lax.axis_size("seq"), lax.axis_size("vocab")
    vocab_local = head_weight.shape[1]
    shard = lax.axis_index("vocab")
    where = jnp.stack([shard // CORES, shard % CORES, shard * vocab_local]).astype(jnp.int32)
    turned = hidden.T
    width = turned.shape[1] // CHUNKS
    first, second = turned[:, :width], turned[:, width:]
    a0 = move(first, turn(1))
    b1 = move(second, turn(-1))
    b0 = move(first, turn(-1))
    weight = prepare(where, head_weight.T, norm_gain.reshape(-1, LANES))
    c0 = move(a0, turn(1))
    a1 = move(second, turn(1))
    c1 = move(b1, turn(-1))
    z0, z1 = move(first, SWAP), move(second, SWAP)
    a0s, b1s, b0s = move(a0, SWAP), move(b1, SWAP), move(b0, SWAP)
    c0s, c1s, a1s = move(c0, SWAP), move(c1, SWAP), move(a1, SWAP)
    near1 = near_head(0, where, weight, (b1, b1s, second, z1))
    near0 = near_head(1, where, weight, (first, z0, a0, a0s))
    teacher = (teacher_ids, teacher_probs)
    earlier, mass = far_head(0, 3, where, weight, *near0, *teacher, (c0, c0s, b0, b0s), None, peers)
    near1 = middle(2, where, weight, *near1, (a1, c1))
    late = (a1s, c1s)
    (copies,) = far_head(
        1, 2, where, weight, *near1, *teacher, late, earlier, peers
    )

    came = lax.all_to_all(copies, "vocab", split_axis=0, concat_axis=0, tiled=True)
    message = losses(plan.T, came, mass, doc_ids.reshape(-1, BLOCK), seq_count)
    came = lax.all_to_all(message, "seq", split_axis=0, concat_axis=0, tiled=True)
    doc_loss, row_lse = finish(came)
    return (doc_loss.reshape(-1), row_lse.reshape(-1))


def solution(mesh):
    return jax.shard_map(
        per_device,
        mesh=mesh,
        in_specs=(
            P("seq", "vocab"),
            P(),
            P(None, "vocab"),
            P("seq", None),
            P("seq", None),
            P("seq"),
            P("seq", None),
        ),
        out_specs=(P(), P("seq")),
        check_vma=False,
    )
```
